768 devices in a mesh: section: 96 (over y_hi, z, core), mp: 8 (over y_lo, x).
Axes of the slice: x: 4, y: 8 (y_hi: 4, y_lo: 2; y = y_hi * 2 + y_lo), z: 12, core: 2. Of those that a mesh axis runs over, the one named last changes fastest.
Arguments:
- arrive_rows: bfloat16 [96, 64, 1024], P('section'), may hold values from -50 to 50
- arrive_grads: bfloat16 [96, 64, 1024], P('section'), may hold values from -6 to 6
- feed_rows: bfloat16 [4, 64, 1024], replicated, may hold values from -50 to 50
- feed_grads: bfloat16 [4, 64, 1024], replicated, may hold values from -6 to 6
- stashed_rows: bfloat16 [96, 5, 64, 1024], P('section'), may hold values from -50 to 50
- slot_order: int32 [96, 5], P('section'), may hold values from 0 to 4, each once within a row
- enter_weight: bfloat16 [96, 1024, 4096], P('section', None, 'mp'), may hold values from -0.1875 to 0.1875
- leave_weight: bfloat16 [96, 4096, 1024], P('section', 'mp'), may hold values from -0.09375 to 0.09375
- norm_gain: bfloat16 [96, 1024], P('section'), may hold values from 0.099609375 to 1.8984375
Outputs:
- depart_rows: bfloat16 [96, 64, 1024], P('section')
- depart_grads: bfloat16 [96, 64, 1024], P('section')
- enter_update: bfloat16 [96, 1024, 4096], P('section', None, 'mp')
- leave_update: bfloat16 [96, 4096, 1024], P('section', 'mp')
- gain_update: float32 [96, 1024], P('section')
The draws below stay inside these ranges and needn't reach their ends.
Inputs may be any that keep to these rules, and one draw needn't show every extreme that they name: `slot_order`: each section's row is a permutation of 0 to 4.
All inputs are finite; a program needn't handle non-finite values.
Results may differ from the reference program's by a relative error of at most 0.025.
Values may be sent and summed in bfloat16 or wider, within the bound.
No kernel may reach another device: no remote copies, remote signals or barrier semaphores. Data moves between devices by JAX's collectives and lax.ppermute only.
A program may use at most 64 MiB of HBM per device.

```python
import jax
import jax.numpy as jnp
from jax import lax

D = 1024
HID = 4096
ROWS = 64
STEPS = 5
SECTIONS = 96


def rough_rows(key, shape):
    keys = jax.random.split(key, 3)
    columns = shape[-1]
    ramp = jnp.arange(columns, dtype=jnp.float32) / columns
    column_log = 0.5 * jax.random.uniform(keys[0], (columns,), jnp.float32)
    row_log = jax.random.uniform(keys[1], shape[:-1] + (1,), jnp.float32)
    values = jax.random.normal(keys[2], shape, jnp.float32)
    column_log = column_log + 0.5 * ramp
    values = jnp.clip(values, -5.0, 5.0)
    return values * jnp.power(10.0, column_log + row_log) / 10.0


def draw_arrive_rows(key, part):
    return rough_rows(jax.random.fold_in(key, 31), (SECTIONS, ROWS, D)).astype(jnp.bfloat16)


def draw_feed_rows(key, part):
    return rough_rows(jax.random.fold_in(key, 37), (STEPS - 1, ROWS, D)).astype(jnp.bfloat16)


def draw_stashed_rows(key, part):
    return rough_rows(jax.random.fold_in(key, 41), (SECTIONS, STEPS, ROWS, D)).astype(jnp.bfloat16)


def block_scale(key, extent, cuts, least, high):
    def one(position, shards_of):
        heights = jax.random.uniform(jax.random.fold_in(jax.random.fold_in(key, 6), position), (shards_of,), jnp.float32, least / len(cuts), high / len(cuts))
        return jnp.repeat(jnp.exp(heights), extent[position] // shards_of).reshape((-1,) + (1,) * (len(extent) - position - 1))

    factor_of = one(*cuts[0])
    for cut in cuts[1:]:
        factor_of = factor_of * one(*cut)
    return factor_of


def noise(key, extent, deviation, most, cuts=(), kind=jnp.bfloat16):
    drawn = deviation * jax.random.normal(key, extent, jnp.float32)
    if cuts:
        drawn = drawn * block_scale(key, extent, cuts, -0.22, 0.18)
    return jnp.clip(drawn, -most, most).astype(kind)


def setup_inputs(seed: int = 0) -> dict:
    key_list = jax.random.split(jax.random.key(seed), 10)
    return {
        "arrive_rows": draw_arrive_rows(jax.random.fold_in(key_list[9], 71), 0),
        "arrive_grads": noise(key_list[1], (SECTIONS, ROWS, D), 1.0, 6.0, ((0, 96),)),
        "feed_rows": draw_feed_rows(jax.random.fold_in(key_list[9], 71), 0),
        "feed_grads": noise(key_list[3], (STEPS - 1, ROWS, D), 1.0, 6.0),
        "stashed_rows": draw_stashed_rows(jax.random.fold_in(key_list[9], 71), 0),
        "slot_order": jax.vmap(lambda own: jax.random.permutation(own, STEPS))(jax.random.split(key_list[5], SECTIONS)).reshape((SECTIONS, STEPS)).astype(jnp.int32),
        "enter_weight": noise(key_list[6], (SECTIONS, D, HID), D ** -0.5, 0.1875, ((0, 96), (2, 8))),
        "leave_weight": noise(key_list[7], (SECTIONS, HID, D), HID ** -0.5, 0.09375, ((0, 96), (1, 8))),
        "norm_gain": jnp.clip(1.0 + 0.18 * jax.random.normal(key_list[8], (SECTIONS, D), jnp.float32), 0.099609375, 1.8984375).astype(jnp.bfloat16),
    }


epsilon = 1e-06

def normalize_project(inputs, weight_in, gain_row):
    inputs_wide = inputs.astype(jnp.float32)
    scaled = (inputs_wide * gain_row.astype(jnp.float32)).astype(jnp.bfloat16)
    squares = lax.optimization_barrier(jnp.sum(inputs_wide * inputs_wide, axis=1))
    inverse = lax.rsqrt(squares / D + epsilon)
    projected = jnp.dot(scaled, weight_in, preferred_element_type=jnp.float32)
    return (scaled, inverse, projected)

def section_forward(operands):
    inputs, weight_in, weight_out, gain_row = operands
    scaled, inverse, projected = normalize_project(inputs, weight_in, gain_row)
    hidden = jax.nn.gelu(inverse[:, None] * projected).astype(jnp.bfloat16)
    branch = jnp.dot(hidden, weight_out, preferred_element_type=jnp.float32)
    return (inputs.astype(jnp.float32) + branch).astype(jnp.bfloat16)

def section_backward(operands):
    inputs, output_grad, weight_in, weight_out, gain_row = operands
    scaled, inverse, projected = normalize_project(inputs, weight_in, gain_row)
    preact = inverse[:, None] * projected
    hidden_wide, slope_fn = jax.vjp(jax.nn.gelu, preact)
    hidden = hidden_wide.astype(jnp.bfloat16)
    hidden_grad = jnp.dot(output_grad, weight_out.T, preferred_element_type=jnp.float32)
    pre_grad = slope_fn(hidden_grad)[0]
    scaled_grad = (inverse[:, None] * pre_grad).astype(jnp.bfloat16)
    inverse_grad = lax.optimization_barrier(jnp.sum(pre_grad * projected, axis=1))
    norm_factor = -inverse_grad * inverse * inverse * inverse / D
    input_part = jnp.dot(scaled_grad, weight_in.T, preferred_element_type=jnp.float32)
    inputs_wide = inputs.astype(jnp.float32)
    input_grad = output_grad.astype(jnp.float32) + input_part * gain_row.astype(jnp.float32) + norm_factor[:, None] * inputs_wide
    gain_part = lax.optimization_barrier(jnp.sum(input_part * inputs_wide, axis=0))
    return (input_grad.astype(jnp.bfloat16), hidden, scaled, scaled_grad, gain_part)

def weight_grads(operands):
    hidden_rows, grad_rows, scaled_rows, update_rows = operands
    leave_total = jnp.dot(hidden_rows.T, grad_rows, preferred_element_type=jnp.float32)
    enter_total = jnp.dot(scaled_rows.T, update_rows, preferred_element_type=jnp.float32)
    return (enter_total.astype(jnp.bfloat16), leave_total.astype(jnp.bfloat16))

def reference(arrive_rows, arrive_grads, feed_rows, feed_grads, stashed_rows, slot_order, enter_weight, leave_weight, norm_gain):
    section_count = arrive_rows.shape[0]
    section_ids = jnp.arange(section_count, dtype=jnp.int32)
    inputs_now = arrive_rows
    grads_now = arrive_grads
    gain_total = jnp.zeros(norm_gain.shape, jnp.float32)
    hidden_steps = []
    grad_steps = []
    scaled_steps = []
    update_steps = []
    outputs = arrive_rows
    input_grad = arrive_grads
    for step in range(STEPS):
        outputs = lax.map(section_forward, (inputs_now, enter_weight, leave_weight, norm_gain))
        picked = stashed_rows[section_ids, slot_order[:, step].astype(jnp.int32)]
        input_grad, hidden, scaled, scaled_grad, gain_part = lax.map(section_backward, (picked, grads_now, enter_weight, leave_weight, norm_gain))
        hidden_steps.append(hidden)
        grad_steps.append(grads_now)
        scaled_steps.append(scaled)
        update_steps.append(scaled_grad)
        gain_total = gain_total + gain_part
        if step + 1 < STEPS:
            inputs_now = jnp.concatenate([feed_rows[step][None], outputs[:-1]], axis=0)
            grads_now = jnp.concatenate([input_grad[1:], feed_grads[step][None]], axis=0)
    stacked = (jnp.concatenate(hidden_steps, axis=1), jnp.concatenate(grad_steps, axis=1), jnp.concatenate(scaled_steps, axis=1), jnp.concatenate(update_steps, axis=1))
    enter_update, leave_update = lax.map(weight_grads, stacked)
    return (outputs, input_grad, enter_update, leave_update, gain_total)
```

```python
import jax
import jax.numpy as jnp
from jax import lax
from jax.sharding import PartitionSpec as P

D = 1024
EPSILON = 1e-06
BOTH = ("section", "mp")


def pair_groups(sections, peers, first):
    groups = []
    for k in range(first, sections + first, 2):
        pair = (k % sections, (k + 1) % sections)
        groups.append([s * peers + m for s in pair for m in range(peers)])
    return groups


def against_rows(left, right):
    return lax.dot_general(
        left, right, (((1,), (1,)), ((), ())), preferred_element_type=jnp.float32
    )


def across_rows(left, right):
    return lax.dot_general(
        left, right, (((0,), (0,)), ((), ())), preferred_element_type=jnp.float32
    )


def local(
    arrive_rows,
    arrive_grads,
    feed_rows,
    feed_grads,
    stashed_rows,
    slot_order,
    enter_weight,
    leave_weight,
    norm_gain,
):
    sections = lax.axis_size("section")
    peers = lax.axis_size("mp")
    position = lax.axis_index("section")
    first_section = position == 0
    last_section = position == sections - 1
    even_pairs = pair_groups(sections, peers, 0)
    odd_pairs = pair_groups(sections, peers, 1)
    weight_in = enter_weight[0]
    weight_out = leave_weight[0]
    gain_row = norm_gain[0].astype(jnp.float32)
    stashed = stashed_rows[0]
    steps, rows = stashed.shape[0], stashed.shape[1]
    share = rows // peers
    portion = 1.0 / peers

    def normalize(rows_in):
        wide = rows_in.astype(jnp.float32)
        scaled = (wide * gain_row).astype(jnp.bfloat16)
        inverse = lax.rsqrt(jnp.sum(wide * wide, axis=1) / D + EPSILON)
        projected = jnp.dot(scaled, weight_in, preferred_element_type=jnp.float32)
        return (wide, scaled, inverse, projected)

    def summed(parts):
        return jnp.sum(parts.astype(jnp.float32), axis=0).astype(jnp.bfloat16)

    inputs = arrive_rows[0]
    grads = arrive_grads[0]
    gain_total = jnp.zeros_like(gain_row)
    hidden_list, grad_list, scaled_list, update_list = [], [], [], []
    for step in range(steps):
        wide, _, inverse, projected = normalize(inputs)
        hidden = jax.nn.gelu(inverse[:, None] * projected).astype(jnp.bfloat16)
        forward = jnp.dot(hidden, weight_out, preferred_element_type=jnp.float32)
        forward = (forward + wide * portion).astype(jnp.bfloat16)

        slot = lax.dynamic_index_in_dim(stashed, slot_order[0, step], 0, keepdims=False)
        slot_wide, slot_scaled, slot_inverse, slot_proj = normalize(slot)
        slot_hidden, slope_fn = jax.vjp(jax.nn.gelu, slot_inverse[:, None] * slot_proj)
        hidden_grad = against_rows(grads, weight_out)
        pre_grad = slope_fn(hidden_grad)[0]
        scaled_grad = (slot_inverse[:, None] * pre_grad).astype(jnp.bfloat16)
        factor = -jnp.sum(pre_grad * slot_proj, axis=1) * slot_inverse**3 / D
        input_part = against_rows(scaled_grad, weight_in)
        gain_total = gain_total + jnp.sum(input_part * slot_wide, axis=0)
        backward = (
            grads.astype(jnp.float32) * portion
            + input_part * gain_row
            + factor[:, None] * slot_wide
        ).astype(jnp.bfloat16)
        hidden_list.append(slot_hidden.astype(jnp.bfloat16))
        grad_list.append(grads)
        scaled_list.append(slot_scaled)
        update_list.append(scaled_grad)

        if step + 1 < steps:
            parts = jnp.concatenate([backward, forward], axis=0).reshape(2 * peers, share, D)
            parts = lax.all_to_all(parts, BOTH, 0, 0, axis_index_groups=odd_pairs, tiled=True)
            low, high = summed(parts[:peers]), summed(parts[peers:])
            spread = (peers, share, D)
            parts = jnp.concatenate(
                [jnp.broadcast_to(low[None], spread), jnp.broadcast_to(high[None], spread)], axis=0
            )
            parts = lax.all_to_all(parts, BOTH, 0, 0, axis_index_groups=even_pairs, tiled=True)
            inputs = jnp.where(first_section, feed_rows[step], parts[:peers].reshape(rows, D))
            grads = jnp.where(last_section, feed_grads[step], parts[peers:].reshape(rows, D))

    gain_high = lax.reduce_precision(gain_total, 8, 7)
    gain_low = gain_total - gain_high
    halves = jnp.stack([gain_high, gain_low]).astype(jnp.bfloat16)
    parts = jnp.concatenate(
        [
            forward.reshape(peers, share, D),
            backward.reshape(peers, share, D),
            jnp.broadcast_to(halves[None], (peers, 2, D)),
            jnp.zeros((peers, share - 2, D), jnp.bfloat16),
        ],
        axis=1,
    )
    parts = lax.all_to_all(parts, "mp", 0, 0, tiled=True)
    gain_total = jnp.sum(parts[:, 2 * share : 2 * share + 2].astype(jnp.float32), axis=(0, 1))
    total = summed(parts[:, : 2 * share])
    parts = lax.all_to_all(
        jnp.broadcast_to(total[None], (peers, 2 * share, D)), "mp", 0, 0, tiled=True
    )
    outputs = parts[:, :share].reshape(rows, D)
    input_grad = parts[:, share:].reshape(rows, D)
    leave_total = across_rows(jnp.concatenate(hidden_list), jnp.concatenate(grad_list))
    enter_total = across_rows(jnp.concatenate(scaled_list), jnp.concatenate(update_list))
    return (
        outputs[None],
        input_grad[None],
        enter_total.astype(jnp.bfloat16)[None],
        leave_total.astype(jnp.bfloat16)[None],
        gain_total[None],
    )


def solution(mesh):
    placed = (
        P("section", None, None),
        P("section", None, None),
        P(),
        P(),
        P("section", None, None, None),
        P("section", None),
        P("section", None, "mp"),
        P("section", "mp", None),
        P("section", None),
    )
    return jax.shard_map(
        local,
        mesh=mesh,
        in_specs=placed,
        out_specs=(
            P("section", None, None),
            P("section", None, None),
            P("section", None, "mp"),
            P("section", "mp", None),
            P("section", None),
        ),
        check_vma=False,
    )
```

```python
import jax
import jax.numpy as jnp
from jax import lax
from jax.experimental import pallas as pl
from jax.experimental.pallas import tpu as pltpu
from jax.sharding import PartitionSpec as P

D = 1024
EPSILON = 1e-06
BOTH = ("section", "mp")
BF16 = jnp.bfloat16
F32 = jnp.float32
LANES = 128
VMEM_LIMIT = 8 << 20
ROOT = 0.7978845608028654
CUBE = 0.044715


def pair_groups(sections, peers, first):
    groups = []
    for k in range(first, sections + first, 2):
        pair = (k % sections, (k + 1) % sections)
        groups.append([s * peers + m for s in pair for m in range(peers)])
    return groups


def times(left, right):
    return jnp.dot(left, right, preferred_element_type=F32)


def against_rows(left, right):
    return lax.dot_general(left, right, (((1,), (1,)), ((), ())), preferred_element_type=F32)


def across_rows(left, right):
    return lax.dot_general(left, right, (((0,), (0,)), ((), ())), preferred_element_type=F32)


def in_vmem(value):
    return pltpu.with_memory_space_constraint(value, pltpu.VMEM)


def call(kernel, outs, args, flops, smem=(), hbm=(), scratch=()):
    space = lambda k: pltpu.SMEM if k in smem else pltpu.HBM if k in hbm else pltpu.VMEM
    return pl.pallas_call(
        kernel,
        out_shape=[
            {"vmem": pltpu.VMEM, "hbm": pltpu.HBM, "any": jax.ShapeDtypeStruct}[place](shape, dtype)
            for shape, dtype, place in outs
        ],
        in_specs=[pl.BlockSpec(memory_space=space(k)) for k in range(len(args))],
        out_specs=[
            pl.BlockSpec(memory_space=pltpu.HBM if place == "hbm" else pltpu.VMEM) for _, _, place in outs
        ],
        scratch_shapes=list(scratch),
        compiler_params=pltpu.CompilerParams(vmem_limit_bytes=VMEM_LIMIT),
        cost_estimate=pl.CostEstimate(flops=flops, transcendentals=0, bytes_accessed=1 << 20),
    )(*args)


def normalize(rows, gain, weight_in):
    scaled = (rows * gain).astype(BF16)
    inverse = lax.rsqrt(jnp.sum(rows * rows, axis=1, keepdims=True) * (1.0 / D) + EPSILON)
    return scaled, inverse, times(scaled, weight_in)


def gelu_parts(preact):
    square = preact * preact
    tanh = jnp.tanh(ROOT * preact * (1.0 + CUBE * square))
    cdf = 0.5 + 0.5 * tanh
    return preact * cdf, cdf, tanh, square


def gelu_slope(preact, cdf, tanh, square):
    return cdf + (0.5 * ROOT) * preact * (1.0 - tanh * tanh) * (1.0 + (3.0 * CUBE) * square)


def flat(ref, peers, start):
    part = ref[start : start + peers].astype(F32)
    return part.reshape(part.shape[0] * part.shape[1], part.shape[2])


def step_kernel(peers, step, last, *refs):
    refs = list(refs)
    take = lambda count: [refs.pop(0) for _ in range(count)]
    plan, stashed = take(2)
    sources = take(1 if step else 2)
    gain_ref, weight_in, weight_out = take(3)
    gains = take(step if last else 0)
    (parts_out,) = take(1)
    targets = take(4 if last else 5)
    slot_ref, *kept = take(6)
    gains_kept = take(len(gains))
    (sems,) = take(1)

    fetches = [pltpu.make_async_copy(stashed.at[plan[0, step]], slot_ref, sems.at[0])]
    fetches += [
        pltpu.make_async_copy(ref, target, sems.at[6 + k]) for k, (ref, target) in enumerate(zip(gains, gains_kept))
    ]
    for fetch in fetches:
        fetch.start()
    stores = [pltpu.make_async_copy(ref, target, sems.at[1 + k]) for k, (ref, target) in enumerate(zip(kept, targets))]

    def keep(which, value):
        kept[which][...] = value
        stores[which].start()

    if step:
        inputs, grads = flat(sources[0], peers, 0), flat(sources[0], peers, peers)
        grads_low = grads.astype(BF16)
    else:
        inputs, grads_low = sources[0][...].astype(F32), sources[1][...]
        grads = grads_low.astype(F32)
    keep(2, grads_low)
    gain = gain_ref[...].astype(F32)
    portion = 1.0 / peers
    share = inputs.shape[0] // peers

    hidden_grad = against_rows(grads_low, weight_out[...])
    _, inverse, projected = normalize(inputs, gain, weight_in[...])

    fetches[0].wait()
    slot = slot_ref[...].astype(F32)
    slot_scaled, slot_inverse, slot_projected = normalize(slot, gain, weight_in[...])
    keep(1, slot_scaled)

    hidden = gelu_parts(inverse * projected)[0].astype(BF16)
    forward = times(hidden, weight_out[...]) + inputs * portion

    slot_preact = slot_inverse * slot_projected
    slot_hidden, *about = gelu_parts(slot_preact)
    keep(0, slot_hidden.astype(BF16))
    pre_grad = hidden_grad * gelu_slope(slot_preact, *about)
    update = (slot_inverse * pre_grad).astype(BF16)
    keep(3, update)
    input_part = against_rows(update, weight_in[...])
    inner = jnp.sum(pre_grad * slot_projected, axis=1, keepdims=True)
    factor = inner * slot_inverse * slot_inverse * slot_inverse * (-1.0 / D)
    gain_sum = jnp.sum(input_part * slot, axis=0, keepdims=True)
    backward = grads * portion + input_part * gain + factor * slot

    forward = forward.reshape(peers, share, D).astype(BF16)
    backward = backward.reshape(peers, share, D).astype(BF16)
    if last:
        parts_out[:peers, :, :D] = forward
        parts_out[peers:, :, :D] = backward
        for fetch, ref in zip(fetches[1:], gains_kept):
            fetch.wait()
            gain_sum = gain_sum + ref[...]
        stack = jnp.concatenate([gain_sum[:, k * LANES : (k + 1) * LANES] for k in range(D // LANES)], axis=0)
        high = stack.astype(BF16)
        low = (stack - high.astype(F32)).astype(BF16)
        for k in range(2 * peers):
            parts_out[k, :, D : D + LANES] = high
            parts_out[k, :, D + LANES :] = low
    else:
        keep(4, gain_sum)
        parts_out[:peers] = backward
        parts_out[peers:] = forward
    for store in stores:
        store.wait()


def sum_kernel(peers, sections, step, received, feed_rows, feed_grads, spread_out):
    position = lax.axis_index("section")
    for start, edge, feed in ((0, 0, feed_rows), (peers, sections - 1, feed_grads)):
        total = received[start].astype(F32)
        for k in range(1, peers):
            total = total + received[start + k].astype(F32)
        total = jnp.where(position == edge, feed[step].astype(F32), total).astype(BF16)
        for k in range(peers):
            spread_out[start + k] = total


def last_sum_kernel(peers, received, spread_out, gain_out):
    for start in (0, peers):
        total = received[start, :, :D].astype(F32)
        for k in range(1, peers):
            total = total + received[start + k, :, :D].astype(F32)
        total = total.astype(BF16)
        for k in range(peers):
            spread_out[start + k] = total
    own = lax.rem(lax.axis_index("section"), 2) * peers
    total = jnp.zeros((D // LANES, LANES), F32)
    for k in range(peers):
        total = total + received[own + k, :, D : D + LANES].astype(F32)
        total = total + received[own + k, :, D + LANES :].astype(F32)
    gain_out[...] = total


def update_kernel(steps, *refs):
    out, left, right = refs[-3:]
    rows = refs[0].shape[0]
    for step in range(steps):
        left[step * rows : (step + 1) * rows, :] = refs[step][...]
        right[step * rows : (step + 1) * rows, :] = refs[steps + step][...]
    out[...] = across_rows(left[...], right[...]).astype(BF16)


def finish_kernel(peers, received, outputs, input_grad):
    outputs[...] = flat(received, peers, 0).astype(BF16)
    input_grad[...] = flat(received, peers, peers).astype(BF16)


def local(
    arrive_rows,
    arrive_grads,
    feed_rows,
    feed_grads,
    stashed_rows,
    slot_order,
    enter_weight,
    leave_weight,
    norm_gain,
):
    sections = lax.axis_size("section")
    peers = lax.axis_size("mp")
    even_pairs = pair_groups(sections, peers, 0)
    odd_pairs = pair_groups(sections, peers, 1)
    weight_in = in_vmem(enter_weight[0])
    weight_out = in_vmem(leave_weight[0])
    gain = in_vmem(norm_gain)
    stashed = pltpu.with_memory_space_constraint(stashed_rows[0], pltpu.HBM)
    steps, rows = stashed.shape[0], stashed.shape[1]
    width = enter_weight.shape[2]
    share = rows // peers
    matmul = 2 * rows * D * width
    own = lax.axis_index("mp") * share
    feeds = [in_vmem(lax.dynamic_slice_in_dim(feed, own, share, 1)) for feed in (feed_rows, feed_grads)]

    def exchange(parts, groups):
        return in_vmem(lax.all_to_all(parts, BOTH, 0, 0, axis_index_groups=groups, tiled=True))

    def spread(kernel, more, *args):
        outs = [((2 * peers, share, D), BF16, "vmem")] + more
        return call(kernel, outs, args, 1 << 18)

    kept = [((rows, width), BF16), ((rows, D), BF16), ((rows, D), BF16), ((rows, width), BF16), ((1, D), F32)]
    source = (in_vmem(arrive_rows[0]), in_vmem(arrive_grads[0]))
    stored = [[] for _ in kept]
    for step in range(steps):
        last = step + 1 == steps
        gains = stored[4] if last else []
        args = [slot_order, stashed, *source, gain, weight_in, weight_out, *gains]
        outs = [((2 * peers, share, D + 2 * LANES if last else D), BF16, "vmem")]
        outs += [(shape, dtype, "hbm") for shape, dtype in kept[: 4 if last else 5]]
        scratch = [pltpu.VMEM((rows, D), BF16), *(pltpu.VMEM(*k) for k in kept), *(pltpu.VMEM((1, D), F32) for _ in gains)]
        scratch.append(pltpu.SemaphoreType.DMA((6 + steps,)))
        kernel = lambda *refs: step_kernel(peers, step, last, *refs)
        in_hbm = [1, *range(len(args) - len(gains), len(args))]
        parts, *results = call(kernel, outs, args, 5 * matmul, smem=(0,), hbm=in_hbm, scratch=scratch)
        for past, result in zip(stored, results):
            past.append(result)
        if last:
            break
        (parts,) = spread(
            lambda *refs: sum_kernel(peers, sections, step, *refs), [], exchange(parts, odd_pairs), *feeds
        )
        source = (exchange(parts, even_pairs),)

    parts, gain_total = spread(
        lambda *refs: last_sum_kernel(peers, *refs),
        [((D // LANES, LANES), F32, "any")],
        exchange(parts, even_pairs),
    )
    received = exchange(parts, even_pairs)
    kernel = lambda *refs: finish_kernel(peers, *refs)
    outputs, input_grad = call(kernel, [((rows, D), BF16, "any")] * 2, (received,), 1 << 18)
    totals = []
    for left, right in ((stored[0], stored[2]), (stored[1], stored[3])):
        shape = (left[0].shape[1], right[0].shape[1])
        scratch = [pltpu.VMEM((steps * rows, n), BF16) for n in shape]
        kernel = lambda *refs: update_kernel(steps, *refs)
        totals += call(kernel, [(shape, BF16, "any")], (*left, *right), steps * matmul, scratch=scratch)
    return (
        outputs[None],
        input_grad[None],
        totals[1][None],
        totals[0][None],
        gain_total.reshape(1, D),
    )


def solution(mesh):
    placed = (
        P("section", None, None),
        P("section", None, None),
        P(),
        P(),
        P("section", None, None, None),
        P("section", None),
        P("section", None, "mp"),
        P("section", "mp", None),
        P("section", None),
    )
    return jax.shard_map(
        local,
        mesh=mesh,
        in_specs=placed,
        out_specs=(
            P("section", None, None),
            P("section", None, None),
            P("section", None, "mp"),
            P("section", "mp", None),
            P("section", None),
        ),
        check_vma=False,
    )
```

```python
import jax
import jax.numpy as jnp
from jax import lax
from jax.experimental import pallas as pl
from jax.experimental.pallas import tpu as pltpu
from jax.sharding import PartitionSpec as P

D = 1024
EPSILON = 1e-06
BOTH = ("section", "mp")
BF16 = jnp.bfloat16
F32 = jnp.float32
LANES = 128
VMEM_LIMIT = 8 << 20
ROOT = 0.7978845608028654
CUBE = 0.044715


def pair_groups(sections, peers, first):
    groups = []
    for k in range(first, sections + first, 2):
        pair = (k % sections, (k + 1) % sections)
        groups.append([s * peers + m for s in pair for m in range(peers)])
    return groups


def times(left, right):
    return jnp.dot(left, right, preferred_element_type=F32)


def against_rows(left, right):
    return lax.dot_general(left, right, (((1,), (1,)), ((), ())), preferred_element_type=F32)


def across_rows(left, right):
    return lax.dot_general(left, right, (((0,), (0,)), ((), ())), preferred_element_type=F32)


def in_vmem(value):
    return pltpu.with_memory_space_constraint(value, pltpu.VMEM)


def call(kernel, outs, args, flops, smem=(), hbm=(), scratch=()):
    space = lambda k: pltpu.SMEM if k in smem else pltpu.HBM if k in hbm else pltpu.VMEM
    return pl.pallas_call(
        kernel,
        out_shape=[
            {"vmem": pltpu.VMEM, "hbm": pltpu.HBM, "any": jax.ShapeDtypeStruct}[place](shape, dtype)
            for shape, dtype, place in outs
        ],
        in_specs=[pl.BlockSpec(memory_space=space(k)) for k in range(len(args))],
        out_specs=[
            pl.BlockSpec(memory_space=pltpu.HBM if place == "hbm" else pltpu.VMEM) for _, _, place in outs
        ],
        scratch_shapes=list(scratch),
        compiler_params=pltpu.CompilerParams(vmem_limit_bytes=VMEM_LIMIT),
        cost_estimate=pl.CostEstimate(flops=flops, transcendentals=0, bytes_accessed=1 << 20),
    )(*args)


def normalize(rows, gain, weight_in):
    scaled = (rows * gain).astype(BF16)
    inverse = lax.rsqrt(jnp.sum(rows * rows, axis=1, keepdims=True) * (1.0 / D) + EPSILON)
    return scaled, inverse, times(scaled, weight_in)


def gelu_parts(preact):
    square = preact * preact
    tanh = jnp.tanh(ROOT * preact * (1.0 + CUBE * square))
    cdf = 0.5 + 0.5 * tanh
    return preact * cdf, cdf, tanh, square


def gelu_slope(preact, cdf, tanh, square):
    return cdf + (0.5 * ROOT) * preact * (1.0 - tanh * tanh) * (1.0 + (3.0 * CUBE) * square)


def flat(ref, peers, start):
    part = ref[start : start + peers].astype(F32)
    return part.reshape(part.shape[0] * part.shape[1], part.shape[2])


def step_kernel(peers, step, last, *refs):
    refs = list(refs)
    take = lambda count: [refs.pop(0) for _ in range(count)]
    first = step == 0
    operands = take(9 if first else 6 + (step if last else 0))
    (parts_out,) = take(1)
    targets = take(4 if last else 5)
    feeds_out = take(2 if first else 0)
    slot_ref, *kept = take(6)
    *held, sems = refs
    count = iter(range(sems.shape[0]))

    def copy(source, target):
        return pltpu.make_async_copy(source, target, sems.at[next(count)])

    def begin(sources, targets):
        copies = [copy(source, target) for source, target in zip(sources, targets)]
        for one in copies:
            one.start()
        return copies

    if first:
        plan_hbm, stashed, rows_hbm, grads_hbm, *more = operands
        plan, rows_ref, grads_ref, gain_ref, weight_in, weight_out = held
        (planned,) = begin([plan_hbm], [plan])
        fetches = begin([grads_hbm, more[2], more[0], rows_hbm, more[1]], [grads_ref, weight_out, gain_ref, rows_ref, weight_in])
        own = pl.multiple_of(lax.axis_index("mp") * feeds_out[0].shape[1], feeds_out[0].shape[1])
        feed_copies = begin([feed.at[:, pl.ds(own, feeds_out[0].shape[1]), :] for feed in more[3:]], feeds_out)
        planned.wait()
        (slot_copy,) = begin([stashed.at[plan[0, step]]], [slot_ref])
        for fetch in fetches:
            fetch.wait()
        inputs, grads_low = rows_ref[...].astype(F32), grads_ref[...]
        grads = grads_low.astype(F32)
    else:
        plan, stashed, received, gain_ref, weight_in, weight_out, *gains = operands
        (slot_copy,) = begin([stashed.at[plan[0, step]]], [slot_ref])
        gain_copies = begin(gains, held)
        inputs, grads = flat(received, peers, 0), flat(received, peers, peers)
        grads_low = grads.astype(BF16)
    stores = [copy(ref, target) for ref, target in zip(kept, targets)]

    def keep(which, value):
        kept[which][...] = value
        stores[which].start()

    keep(2, grads_low)
    gain = gain_ref[...].astype(F32)
    portion = 1.0 / peers
    share = inputs.shape[0] // peers

    hidden_grad = against_rows(grads_low, weight_out[...])
    _, inverse, projected = normalize(inputs, gain, weight_in[...])

    slot_copy.wait()
    slot = slot_ref[...].astype(F32)
    slot_scaled, slot_inverse, slot_projected = normalize(slot, gain, weight_in[...])
    keep(1, slot_scaled)

    slot_preact = slot_inverse * slot_projected
    slot_hidden, *about = gelu_parts(slot_preact)
    keep(0, slot_hidden.astype(BF16))
    pre_grad = hidden_grad * gelu_slope(slot_preact, *about)
    update = (slot_inverse * pre_grad).astype(BF16)
    keep(3, update)
    input_part = against_rows(update, weight_in[...])
    inner = jnp.sum(pre_grad * slot_projected, axis=1, keepdims=True)
    factor = inner * slot_inverse * slot_inverse * slot_inverse * (-1.0 / D)
    gain_sum = jnp.sum(input_part * slot, axis=0, keepdims=True)
    if not last:
        keep(4, gain_sum)
    backward = grads * portion + input_part * gain + factor * slot
    backward = backward.reshape(peers, share, D).astype(BF16)

    hidden = gelu_parts(inverse * projected)[0].astype(BF16)
    forward = times(hidden, weight_out[...]) + inputs * portion
    forward = forward.reshape(peers, share, D).astype(BF16)
    if last:
        parts_out[:peers, :, :D] = forward
        parts_out[peers:, :, :D] = backward
        for fetch, ref in zip(gain_copies, held):
            fetch.wait()
            gain_sum = gain_sum + ref[...]
        stack = jnp.concatenate([gain_sum[:, k * LANES : (k + 1) * LANES] for k in range(D // LANES)], axis=0)
        high = stack.astype(BF16)
        low = (stack - high.astype(F32)).astype(BF16)
        for k in range(2 * peers):
            parts_out[k, :, D : D + LANES] = high
            parts_out[k, :, D + LANES :] = low
    else:
        parts_out[:peers] = backward
        parts_out[peers:] = forward
    for store in stores:
        store.wait()
    if first:
        for fetch in feed_copies:
            fetch.wait()


def sum_kernel(peers, sections, step, received, feed_rows, feed_grads, spread_out):
    position = lax.axis_index("section")
    for start, edge, feed in ((0, 0, feed_rows), (peers, sections - 1, feed_grads)):
        total = received[start].astype(F32)
        for k in range(1, peers):
            total = total + received[start + k].astype(F32)
        total = jnp.where(position == edge, feed[step].astype(F32), total).astype(BF16)
        for k in range(peers):
            spread_out[start + k] = total


def last_sum_kernel(peers, received, spread_out, gain_out):
    for start in (0, peers):
        total = received[start, :, :D].astype(F32)
        for k in range(1, peers):
            total = total + received[start + k, :, :D].astype(F32)
        total = total.astype(BF16)
        for k in range(peers):
            spread_out[start + k] = total
    own = lax.rem(lax.axis_index("section"), 2) * peers
    total = jnp.zeros((D // LANES, LANES), F32)
    for k in range(peers):
        total = total + received[own + k, :, D : D + LANES].astype(F32)
        total = total + received[own + k, :, D + LANES :].astype(F32)
    gain_out[...] = total


def update_kernel(steps, *refs):
    out, left, right = refs[-3:]
    rows = refs[0].shape[0]
    for step in range(steps):
        left[step * rows : (step + 1) * rows, :] = refs[step][...]
        right[step * rows : (step + 1) * rows, :] = refs[steps + step][...]
    out[...] = across_rows(left[...], right[...]).astype(BF16)


def finish_kernel(peers, received, outputs, input_grad):
    outputs[...] = flat(received, peers, 0).astype(BF16)
    input_grad[...] = flat(received, peers, peers).astype(BF16)


def local(
    arrive_rows,
    arrive_grads,
    feed_rows,
    feed_grads,
    stashed_rows,
    slot_order,
    enter_weight,
    leave_weight,
    norm_gain,
):
    sections = lax.axis_size("section")
    peers = lax.axis_size("mp")
    even_pairs = pair_groups(sections, peers, 0)
    odd_pairs = pair_groups(sections, peers, 1)
    in_hbm = lambda value: pltpu.with_memory_space_constraint(value, pltpu.HBM)
    weights = (enter_weight[0], leave_weight[0])
    stashed = in_hbm(stashed_rows[0])
    steps, rows = stashed.shape[0], stashed.shape[1]
    width = enter_weight.shape[2]
    share = rows // peers
    matmul = 2 * rows * D * width

    def exchange(parts, groups):
        return in_vmem(lax.all_to_all(parts, BOTH, 0, 0, axis_index_groups=groups, tiled=True))

    def spread(kernel, more, *args):
        outs = [((2 * peers, share, D), BF16, "vmem")] + more
        return call(kernel, outs, args, 1 << 18)

    kept = [((rows, width), BF16), ((rows, D), BF16), ((rows, D), BF16), ((rows, width), BF16), ((1, D), F32)]
    stored = [[] for _ in kept]
    for step in range(steps):
        first, last = step == 0, step + 1 == steps
        outs = [((2 * peers, share, D + 2 * LANES if last else D), BF16, "vmem")]
        outs += [(shape, dtype, "hbm") for shape, dtype in kept[: 4 if last else 5]]
        scratch = [pltpu.VMEM((rows, D), BF16), *(pltpu.VMEM(*k) for k in kept)]
        if first:
            args = [slot_order, stashed, arrive_rows[0], arrive_grads[0], norm_gain, *weights, feed_rows, feed_grads]
            args = [in_hbm(arg) for arg in args]
            places = {"hbm": range(len(args))}
            outs += [((steps - 1, share, D), BF16, "vmem")] * 2
            scratch += [pltpu.SMEM(slot_order.shape, jnp.int32)]
            scratch += [pltpu.VMEM(arg.shape, BF16) for arg in args[2:7]]
        else:
            gains = [in_hbm(part) for part in stored[4]] if last else []
            args = [slot_order, stashed, source, in_vmem(norm_gain), *map(in_vmem, weights), *gains]
            places = {"smem": (0,), "hbm": (1, *range(6, len(args)))}
            scratch += [pltpu.VMEM((1, D), F32) for _ in gains]
        scratch.append(pltpu.SemaphoreType.DMA((16,)))
        kernel = lambda *refs: step_kernel(peers, step, last, *refs)
        parts, *results = call(kernel, outs, args, 5 * matmul, scratch=scratch, **places)
        if first:
            *results, feed_inputs, feed_losses = results
        for past, result in zip(stored, results):
            past.append(result)
        if last:
            break
        kernel = lambda *refs: sum_kernel(peers, sections, step, *refs)
        (parts,) = spread(kernel, [], exchange(parts, odd_pairs), feed_inputs, feed_losses)
        source = exchange(parts, even_pairs)
    received = exchange(parts, even_pairs)

    parts, gain_total = spread(
        lambda *refs: last_sum_kernel(peers, *refs),
        [((D // LANES, LANES), F32, "any")],
        received,
    )
    received = exchange(parts, even_pairs)
    kernel = lambda *refs: finish_kernel(peers, *refs)
    outputs, input_grad = call(kernel, [((rows, D), BF16, "any")] * 2, (received,), 1 << 18)
    totals = []
    for left, right in ((stored[0], stored[2]), (stored[1], stored[3])):
        shape = (left[0].shape[1], right[0].shape[1])
        scratch = [pltpu.VMEM((steps * rows, n), BF16) for n in shape]
        kernel = lambda *refs: update_kernel(steps, *refs)
        totals += call(kernel, [(shape, BF16, "any")], (*left, *right), steps * matmul, scratch=scratch)
    return (
        outputs[None],
        input_grad[None],
        totals[1][None],
        totals[0][None],
        gain_total.reshape(1, D),
    )


def solution(mesh):
    placed = (
        P("section", None, None),
        P("section", None, None),
        P(),
        P(),
        P("section", None, None, None),
        P("section", None),
        P("section", None, "mp"),
        P("section", "mp", None),
        P("section", None),
    )
    return jax.shard_map(
        local,
        mesh=mesh,
        in_specs=placed,
        out_specs=(
            P("section", None, None),
            P("section", None, None),
            P("section", None, "mp"),
            P("section", "mp", None),
            P("section", None),
        ),
        check_vma=False,
    )
```

```python
import jax
import jax.numpy as jnp
from jax import lax
from jax.experimental import pallas as pl
from jax.experimental.pallas import tpu as pltpu
from jax.sharding import PartitionSpec as P

D = 1024
EPSILON = 1e-06
BOTH = ("section", "mp")
BF16 = jnp.bfloat16
F32 = jnp.float32
LANES = 128
VMEM_LIMIT = 8 << 20
ROOT = 0.7978845608028654
CUBE = 0.044715


def pair_groups(sections, peers, first):
    groups = []
    for k in range(first, sections + first, 2):
        pair = (k % sections, (k + 1) % sections)
        groups.append([s * peers + m for s in pair for m in range(peers)])
    return groups


def times(left, right):
    return jnp.dot(left, right, preferred_element_type=F32)


def against_rows(left, right):
    return lax.dot_general(left, right, (((1,), (1,)), ((), ())), preferred_element_type=F32)


def across_rows(left, right):
    return lax.dot_general(left, right, (((0,), (0,)), ((), ())), preferred_element_type=F32)


def in_vmem(value):
    return pltpu.with_memory_space_constraint(value, pltpu.VMEM)


def call(kernel, outs, args, flops, smem=(), hbm=(), scratch=()):
    space = lambda k: pltpu.SMEM if k in smem else pltpu.HBM if k in hbm else pltpu.VMEM
    return pl.pallas_call(
        kernel,
        out_shape=[
            {"vmem": pltpu.VMEM, "hbm": pltpu.HBM, "any": jax.ShapeDtypeStruct}[place](shape, dtype)
            for shape, dtype, place in outs
        ],
        in_specs=[pl.BlockSpec(memory_space=space(k)) for k in range(len(args))],
        out_specs=[
            pl.BlockSpec(memory_space=pltpu.HBM if place == "hbm" else pltpu.VMEM) for _, _, place in outs
        ],
        scratch_shapes=list(scratch),
        compiler_params=pltpu.CompilerParams(vmem_limit_bytes=VMEM_LIMIT),
        cost_estimate=pl.CostEstimate(flops=flops, transcendentals=0, bytes_accessed=1 << 20),
    )(*args)


def normalize(rows, gain, weight_in):
    scaled = (rows * gain).astype(BF16)
    inverse = lax.rsqrt(jnp.sum(rows * rows, axis=1, keepdims=True) * (1.0 / D) + EPSILON)
    return scaled, inverse, times(scaled, weight_in)


def gelu_parts(preact):
    square = preact * preact
    tanh = jnp.tanh(ROOT * preact * (1.0 + CUBE * square))
    cdf = 0.5 + 0.5 * tanh
    return preact * cdf, cdf, tanh, square


def gelu_slope(preact, cdf, tanh, square):
    return cdf + (0.5 * ROOT) * preact * (1.0 - tanh * tanh) * (1.0 + (3.0 * CUBE) * square)


def flat(ref, peers, start):
    part = ref[start : start + peers].astype(F32)
    return part.reshape(part.shape[0] * part.shape[1], part.shape[2])


def first_kernel(peers, *refs):
    plan_hbm, stashed, rows_hbm, grads_hbm, gain_hbm, weight_in_hbm, weight_out_hbm, *feeds = refs[:9]
    parts_out, *kept = refs[9:15]
    feeds_out = refs[15:17]
    later = refs[17:-8]
    plan, rows_ref, grads_ref, gain_ref, weight_in, weight_out, slot_ref, sems = refs[-8:]
    count = iter(range(sems.shape[0]))

    def begin(source, target):
        copy = pltpu.make_async_copy(source, target, sems.at[next(count)])
        copy.start()
        return copy

    planned = begin(plan_hbm, plan)
    fetches = [
        begin(grads_hbm, grads_ref),
        begin(weight_out_hbm, weight_out),
        begin(gain_hbm, gain_ref),
        begin(rows_hbm, rows_ref),
        begin(weight_in_hbm, weight_in),
    ]
    share = feeds_out[0].shape[1]
    own = pl.multiple_of(lax.axis_index("mp") * share, share)
    others = [begin(feed.at[:, pl.ds(own, share), :], target) for feed, target in zip(feeds, feeds_out)]
    planned.wait()
    fetches.append(begin(stashed.at[plan[0, 0]], slot_ref))
    others += [begin(stashed.at[plan[0, 1 + k]], target) for k, target in enumerate(later)]
    for fetch in fetches:
        fetch.wait()
    inputs, grads_low = rows_ref[...].astype(F32), grads_ref[...]
    results = both_ways(peers, inputs, grads_low.astype(F32), grads_low, slot_ref, gain_ref, weight_in, weight_out, kept)
    place(peers, parts_out, *results[:2])
    kept[4][...] = results[2]
    for other in others:
        other.wait()


def later_kernel(peers, last, *refs):
    received, slot_ref, gain_ref, weight_in, weight_out, *gains = refs[: -5 if last else -6]
    parts_out, *kept = refs[-5 if last else -6 :]
    inputs, grads = flat(received, peers, 0), flat(received, peers, peers)
    forward, backward, gain_sum = both_ways(
        peers, inputs, grads, grads.astype(BF16), slot_ref, gain_ref, weight_in, weight_out, kept
    )
    if not last:
        place(peers, parts_out, forward, backward)
        kept[4][...] = gain_sum
        return
    parts_out[:peers, :, :D] = forward
    parts_out[peers:, :, :D] = backward
    for ref in gains:
        gain_sum = gain_sum + ref[...]
    stack = jnp.concatenate([gain_sum[:, k * LANES : (k + 1) * LANES] for k in range(D // LANES)], axis=0)
    high = stack.astype(BF16)
    low = (stack - high.astype(F32)).astype(BF16)
    for k in range(2 * peers):
        parts_out[k, :, D : D + LANES] = high
        parts_out[k, :, D + LANES :] = low


def place(peers, parts_out, forward, backward):
    parts_out[:peers] = backward
    parts_out[peers:] = forward


def both_ways(peers, inputs, grads, grads_low, slot_ref, gain_ref, weight_in, weight_out, kept):
    hidden_out, scaled_out, grads_out, update_out = kept[:4]
    grads_out[...] = grads_low
    gain = gain_ref[...].astype(F32)
    portion = 1.0 / peers
    share = inputs.shape[0] // peers

    hidden_grad = against_rows(grads_low, weight_out[...])
    _, inverse, projected = normalize(inputs, gain, weight_in[...])
    slot = slot_ref[...].astype(F32)
    slot_scaled, slot_inverse, slot_projected = normalize(slot, gain, weight_in[...])
    scaled_out[...] = slot_scaled

    slot_preact = slot_inverse * slot_projected
    slot_hidden, *about = gelu_parts(slot_preact)
    hidden_out[...] = slot_hidden.astype(BF16)
    pre_grad = hidden_grad * gelu_slope(slot_preact, *about)
    update = (slot_inverse * pre_grad).astype(BF16)
    update_out[...] = update
    input_part = against_rows(update, weight_in[...])
    inner = jnp.sum(pre_grad * slot_projected, axis=1, keepdims=True)
    factor = inner * slot_inverse * slot_inverse * slot_inverse * (-1.0 / D)
    gain_sum = jnp.sum(input_part * slot, axis=0, keepdims=True)
    backward = grads * portion + input_part * gain + factor * slot
    backward = backward.reshape(peers, share, D).astype(BF16)

    hidden = gelu_parts(inverse * projected)[0].astype(BF16)
    forward = times(hidden, weight_out[...]) + inputs * portion
    forward = forward.reshape(peers, share, D).astype(BF16)
    return forward, backward, gain_sum


def sum_kernel(peers, sections, step, received, feed_rows, feed_grads, spread_out):
    position = lax.axis_index("section")
    for start, edge, feed in ((0, 0, feed_rows), (peers, sections - 1, feed_grads)):
        total = received[start].astype(F32)
        for k in range(1, peers):
            total = total + received[start + k].astype(F32)
        total = jnp.where(position == edge, feed[step].astype(F32), total).astype(BF16)
        for k in range(peers):
            spread_out[start + k] = total


def last_sum_kernel(peers, received, spread_out, gain_out):
    for start in (0, peers):
        total = received[start, :, :D].astype(F32)
        for k in range(1, peers):
            total = total + received[start + k, :, :D].astype(F32)
        total = total.astype(BF16)
        for k in range(peers):
            spread_out[start + k] = total
    own = lax.rem(lax.axis_index("section"), 2) * peers
    total = jnp.zeros((D // LANES, LANES), F32)
    for k in range(peers):
        total = total + received[own + k, :, D : D + LANES].astype(F32)
        total = total + received[own + k, :, D + LANES :].astype(F32)
    gain_out[...] = total


def update_kernel(steps, *refs):
    out, left, right = refs[-3:]
    rows = refs[0].shape[0]
    for step in range(steps):
        left[step * rows : (step + 1) * rows, :] = refs[step][...]
        right[step * rows : (step + 1) * rows, :] = refs[steps + step][...]
    out[...] = across_rows(left[...], right[...]).astype(BF16)


def finish_kernel(peers, received, outputs, input_grad):
    outputs[...] = flat(received, peers, 0).astype(BF16)
    input_grad[...] = flat(received, peers, peers).astype(BF16)


def local(
    arrive_rows,
    arrive_grads,
    feed_rows,
    feed_grads,
    stashed_rows,
    slot_order,
    enter_weight,
    leave_weight,
    norm_gain,
):
    sections = lax.axis_size("section")
    peers = lax.axis_size("mp")
    even_pairs = pair_groups(sections, peers, 0)
    odd_pairs = pair_groups(sections, peers, 1)
    in_hbm = lambda value: pltpu.with_memory_space_constraint(value, pltpu.HBM)
    weights = (enter_weight[0], leave_weight[0])
    stashed = in_hbm(stashed_rows[0])
    steps, rows = stashed.shape[0], stashed.shape[1]
    width = enter_weight.shape[2]
    share = rows // peers
    matmul = 2 * rows * D * width

    def exchange(parts, groups):
        return in_vmem(lax.all_to_all(parts, BOTH, 0, 0, axis_index_groups=groups, tiled=True))

    def spread(kernel, more, *args):
        outs = [((2 * peers, share, D), BF16, "vmem")] + more
        return call(kernel, outs, args, 1 << 18)

    kept = [((rows, width), BF16), ((rows, D), BF16), ((rows, D), BF16), ((rows, width), BF16), ((1, D), F32)]
    stored = [[] for _ in kept]
    for step in range(steps):
        last = step + 1 == steps
        outs = [((2 * peers, share, D + 2 * LANES if last else D), BF16, "vmem")]
        outs += [(shape, dtype, "vmem") for shape, dtype in kept[: 4 if last else 5]]
        if step == 0:
            args = [slot_order, stashed, arrive_rows[0], arrive_grads[0], norm_gain, *weights, feed_rows, feed_grads]
            args = [in_hbm(arg) for arg in args]
            outs += [((steps - 1, share, D), BF16, "vmem")] * 2
            outs += [((rows, D), BF16, "vmem")] * (steps - 1)
            scratch = [pltpu.SMEM(slot_order.shape, jnp.int32)]
            scratch += [pltpu.VMEM(arg.shape, BF16) for arg in args[2:7]]
            scratch += [pltpu.VMEM((rows, D), BF16), pltpu.SemaphoreType.DMA((8 + steps,))]
            kernel = lambda *refs: first_kernel(peers, *refs)
            parts, *results = call(kernel, outs, args, 5 * matmul, hbm=range(len(args)), scratch=scratch)
            feeds, later = results[5:7], results[7:]
        else:
            args = [source, later[step - 1], in_vmem(norm_gain), *map(in_vmem, weights)]
            args += stored[4] if last else []
            kernel = lambda *refs: later_kernel(peers, last, *refs)
            parts, *results = call(kernel, outs, args, 5 * matmul)
        for past, result in zip(stored, results):
            past.append(result)
        if last:
            break
        kernel = lambda *refs: sum_kernel(peers, sections, step, *refs)
        (parts,) = spread(kernel, [], exchange(parts, odd_pairs), *feeds)
        source = exchange(parts, even_pairs)
    received = exchange(parts, even_pairs)

    parts, gain_total = spread(
        lambda *refs: last_sum_kernel(peers, *refs),
        [((D // LANES, LANES), F32, "any")],
        received,
    )
    received = exchange(parts, even_pairs)
    kernel = lambda *refs: finish_kernel(peers, *refs)
    outputs, input_grad = call(kernel, [((rows, D), BF16, "any")] * 2, (received,), 1 << 18)
    totals = []
    for left, right in ((stored[0], stored[2]), (stored[1], stored[3])):
        shape = (left[0].shape[1], right[0].shape[1])
        scratch = [pltpu.VMEM((steps * rows, n), BF16) for n in shape]
        kernel = lambda *refs: update_kernel(steps, *refs)
        totals += call(kernel, [(shape, BF16, "any")], (*left, *right), steps * matmul, scratch=scratch)
    return (
        outputs[None],
        input_grad[None],
        totals[1][None],
        totals[0][None],
        gain_total.reshape(1, D),
    )


def solution(mesh):
    placed = (
        P("section", None, None),
        P("section", None, None),
        P(),
        P(),
        P("section", None, None, None),
        P("section", None),
        P("section", None, "mp"),
        P("section", "mp", None),
        P("section", None),
    )
    return jax.shard_map(
        local,
        mesh=mesh,
        in_specs=placed,
        out_specs=(
            P("section", None, None),
            P("section", None, None),
            P("section", None, "mp"),
            P("section", "mp", None),
            P("section", None),
        ),
        check_vma=False,
    )
```

```python
import jax
import jax.numpy as jnp
from jax import lax
from jax.experimental import pallas as pl
from jax.experimental.pallas import tpu as pltpu
from jax.sharding import PartitionSpec as P

D = 1024
EPSILON = 1e-06
BOTH = ("section", "mp")
BF16 = jnp.bfloat16
F32 = jnp.float32
LANES = 128
VMEM_LIMIT = 8 << 20
ROOT = 0.7978845608028654
CUBE = 0.044715


def pair_groups(sections, peers, first):
    groups = []
    for k in range(first, sections + first, 2):
        pair = (k % sections, (k + 1) % sections)
        groups.append([s * peers + m for s in pair for m in range(peers)])
    return groups


def times(left, right):
    return jnp.dot(left, right, preferred_element_type=F32)


def against_rows(left, right):
    return lax.dot_general(left, right, (((1,), (1,)), ((), ())), preferred_element_type=F32)


def across_rows(left, right):
    return lax.dot_general(left, right, (((0,), (0,)), ((), ())), preferred_element_type=F32)


def in_vmem(value):
    return pltpu.with_memory_space_constraint(value, pltpu.VMEM)


def call(kernel, outs, args, flops, smem=(), hbm=(), scratch=()):
    space = lambda k: pltpu.SMEM if k in smem else pltpu.HBM if k in hbm else pltpu.VMEM
    return pl.pallas_call(
        kernel,
        out_shape=[
            {"vmem": pltpu.VMEM, "hbm": pltpu.HBM, "any": jax.ShapeDtypeStruct}[place](shape, dtype)
            for shape, dtype, place in outs
        ],
        in_specs=[pl.BlockSpec(memory_space=space(k)) for k in range(len(args))],
        out_specs=[
            pl.BlockSpec(memory_space=pltpu.HBM if place == "hbm" else pltpu.VMEM) for _, _, place in outs
        ],
        scratch_shapes=list(scratch),
        compiler_params=pltpu.CompilerParams(vmem_limit_bytes=VMEM_LIMIT),
        cost_estimate=pl.CostEstimate(flops=flops, transcendentals=0, bytes_accessed=1 << 20),
    )(*args)


def normalize(rows, gain, weight_in):
    scaled = (rows * gain).astype(BF16)
    inverse = lax.rsqrt(jnp.sum(rows * rows, axis=1, keepdims=True) * (1.0 / D) + EPSILON)
    return scaled, inverse, times(scaled, weight_in)


def gelu_parts(preact):
    square = preact * preact
    tanh = jnp.tanh(ROOT * preact * (1.0 + CUBE * square))
    cdf = 0.5 + 0.5 * tanh
    return preact * cdf, cdf, tanh, square


def gelu_slope(preact, cdf, tanh, square):
    return cdf + (0.5 * ROOT) * preact * (1.0 - tanh * tanh) * (1.0 + (3.0 * CUBE) * square)


def flat(part):
    return part.astype(F32).reshape(part.shape[0] * part.shape[1], part.shape[2])


def first_kernel(peers, *refs):
    plan_hbm, stashed, rows_hbm, grads_hbm, gain_hbm, weight_in_hbm, weight_out_hbm, *feeds = refs[:9]
    parts_out, *kept = refs[9:15]
    feeds_out = refs[15:17]
    later = refs[17:-8]
    plan, rows_ref, grads_ref, gain_ref, weight_in, weight_out, slot_ref, sems = refs[-8:]
    count = iter(range(sems.shape[0]))

    def begin(source, target):
        copy = pltpu.make_async_copy(source, target, sems.at[next(count)])
        copy.start()
        return copy

    planned = begin(plan_hbm, plan)
    fetches = [
        begin(grads_hbm, grads_ref),
        begin(weight_out_hbm, weight_out),
        begin(gain_hbm, gain_ref),
        begin(rows_hbm, rows_ref),
        begin(weight_in_hbm, weight_in),
    ]
    share = feeds_out[0].shape[1]
    own = pl.multiple_of(lax.axis_index("mp") * share, share)
    others = [begin(feed.at[:, pl.ds(own, share), :], target) for feed, target in zip(feeds, feeds_out)]
    planned.wait()
    fetches.append(begin(stashed.at[plan[0, 0]], slot_ref))
    others += [begin(stashed.at[plan[0, 1 + k]], target) for k, target in enumerate(later)]

    def load_grads():
        for fetch in fetches[:2]:
            fetch.wait()
        return grads_ref[...].astype(F32)

    def load_inputs():
        for fetch in fetches[2:5]:
            fetch.wait()
        return rows_ref[...].astype(F32)

    def load_slot():
        fetches[5].wait()
        return slot_ref[...].astype(F32)

    results = both_ways(peers, load_grads, load_inputs, load_slot, gain_ref, weight_in, weight_out, kept)
    place(peers, parts_out, *results[:2])
    kept[4][...] = results[2]
    for other in others:
        other.wait()


def later_kernel(peers, last, *refs):
    received, slot_ref, gain_ref, weight_in, weight_out, *gains = refs[: -5 if last else -6]
    parts_out, *kept = refs[-5 if last else -6 :]
    forward, backward, gain_sum = both_ways(
        peers,
        lambda: flat(received[peers:]),
        lambda: flat(received[:peers]),
        lambda: slot_ref[...].astype(F32),
        gain_ref,
        weight_in,
        weight_out,
        kept,
    )
    if not last:
        place(peers, parts_out, forward, backward)
        kept[4][...] = gain_sum
        return
    share = forward.shape[1]
    parts_out[:, :share, :D] = forward
    parts_out[:, share:, :D] = backward
    for ref in gains:
        gain_sum = gain_sum + ref[...]
    stack = jnp.concatenate([gain_sum[:, k * LANES : (k + 1) * LANES] for k in range(D // LANES)], axis=0)
    high = stack.astype(BF16)
    low = (stack - high.astype(F32)).astype(BF16)
    for k in range(peers):
        parts_out[k, :share, D:] = high
        parts_out[k, share:, D:] = low


def place(peers, parts_out, forward, backward):
    parts_out[:peers] = backward
    parts_out[peers:] = forward


def both_ways(peers, load_grads, load_inputs, load_slot, gain_ref, weight_in, weight_out, kept):
    hidden_out, scaled_out, grads_out, update_out = kept[:4]
    grads = load_grads()
    grads_low = grads.astype(BF16)
    grads_out[...] = grads_low
    hidden_grad = against_rows(grads_low, weight_out[...])
    inputs = load_inputs()
    gain = gain_ref[...].astype(F32)
    portion = 1.0 / peers
    share = inputs.shape[0] // peers
    _, inverse, projected = normalize(inputs, gain, weight_in[...])
    slot = load_slot()
    slot_scaled, slot_inverse, slot_projected = normalize(slot, gain, weight_in[...])
    scaled_out[...] = slot_scaled

    slot_preact = slot_inverse * slot_projected
    slot_hidden, *about = gelu_parts(slot_preact)
    hidden_out[...] = slot_hidden.astype(BF16)
    pre_grad = hidden_grad * gelu_slope(slot_preact, *about)
    update = (slot_inverse * pre_grad).astype(BF16)
    update_out[...] = update
    input_part = against_rows(update, weight_in[...])
    inner = jnp.sum(pre_grad * slot_projected, axis=1, keepdims=True)
    factor = inner * slot_inverse * slot_inverse * slot_inverse * (-1.0 / D)
    gain_sum = jnp.sum(input_part * slot, axis=0, keepdims=True)
    backward = grads * portion + input_part * gain + factor * slot
    backward = backward.reshape(peers, share, D).astype(BF16)

    hidden = gelu_parts(inverse * projected)[0].astype(BF16)
    forward = times(hidden, weight_out[...]) + inputs * portion
    forward = forward.reshape(peers, share, D).astype(BF16)
    return forward, backward, gain_sum


def sum_kernel(peers, sections, step, received, feed_rows, feed_grads, spread_out):
    position = lax.axis_index("section")
    for start, edge, feed in ((0, 0, feed_rows), (peers, sections - 1, feed_grads)):
        total = received[start].astype(F32)
        for k in range(1, peers):
            total = total + received[start + k].astype(F32)
        total = jnp.where(position == edge, feed[step].astype(F32), total).astype(BF16)
        for k in range(peers):
            spread_out[start + k] = total


def last_sum_kernel(peers, received, spread_out, gain_out):
    total = received[0].astype(F32)
    for k in range(1, peers):
        total = total + received[k].astype(F32)
    piece = total[:, :D].astype(BF16)
    for k in range(peers):
        spread_out[k] = piece
    share = total.shape[0] // 2
    gain_out[...] = total[:share, D:] + total[share:, D:]


def update_kernel(steps, *refs):
    out, left, right = refs[-3:]
    rows = refs[0].shape[0]
    for step in range(steps):
        left[step * rows : (step + 1) * rows, :] = refs[step][...]
        right[step * rows : (step + 1) * rows, :] = refs[steps + step][...]
    out[...] = across_rows(left[...], right[...]).astype(BF16)


def finish_kernel(received, outputs, input_grad):
    share = received.shape[1] // 2
    outputs[...] = flat(received[:, :share]).astype(BF16)
    input_grad[...] = flat(received[:, share:]).astype(BF16)


def local(
    arrive_rows,
    arrive_grads,
    feed_rows,
    feed_grads,
    stashed_rows,
    slot_order,
    enter_weight,
    leave_weight,
    norm_gain,
):
    sections = lax.axis_size("section")
    peers = lax.axis_size("mp")
    even_pairs = pair_groups(sections, peers, 0)
    odd_pairs = pair_groups(sections, peers, 1)
    in_hbm = lambda value: pltpu.with_memory_space_constraint(value, pltpu.HBM)
    weights = (enter_weight[0], leave_weight[0])
    stashed = in_hbm(stashed_rows[0])
    steps, rows = stashed.shape[0], stashed.shape[1]
    width = enter_weight.shape[2]
    share = rows // peers
    matmul = 2 * rows * D * width

    def exchange(parts, groups):
        return in_vmem(lax.all_to_all(parts, BOTH, 0, 0, axis_index_groups=groups, tiled=True))

    def exchange_within(parts):
        return in_vmem(lax.all_to_all(parts, "mp", 0, 0, tiled=True))

    kept = [((rows, width), BF16), ((rows, D), BF16), ((rows, D), BF16), ((rows, width), BF16), ((1, D), F32)]
    stored = [[] for _ in kept]
    for step in range(steps):
        last = step + 1 == steps
        whole = (peers, 2 * share, D + LANES) if last else (2 * peers, share, D)
        outs = [(whole, BF16, "vmem")]
        outs += [(shape, dtype, "vmem") for shape, dtype in kept[: 4 if last else 5]]
        if step == 0:
            args = [slot_order, stashed, arrive_rows[0], arrive_grads[0], norm_gain, *weights, feed_rows, feed_grads]
            args = [in_hbm(arg) for arg in args]
            outs += [((steps - 1, share, D), BF16, "vmem")] * 2
            outs += [((rows, D), BF16, "vmem")] * (steps - 1)
            scratch = [pltpu.SMEM(slot_order.shape, jnp.int32)]
            scratch += [pltpu.VMEM(arg.shape, BF16) for arg in args[2:7]]
            scratch += [pltpu.VMEM((rows, D), BF16), pltpu.SemaphoreType.DMA((8 + steps,))]
            kernel = lambda *refs: first_kernel(peers, *refs)
            parts, *results = call(kernel, outs, args, 5 * matmul, hbm=range(len(args)), scratch=scratch)
            feeds, later = results[5:7], results[7:]
        else:
            args = [source, later[step - 1], in_vmem(norm_gain), *map(in_vmem, weights)]
            args += stored[4] if last else []
            kernel = lambda *refs: later_kernel(peers, last, *refs)
            parts, *results = call(kernel, outs, args, 5 * matmul)
        for past, result in zip(stored, results):
            past.append(result)
        if last:
            break
        kernel = lambda *refs: sum_kernel(peers, sections, step, *refs)
        args = (exchange(parts, odd_pairs), *feeds)
        (parts,) = call(kernel, [((2 * peers, share, D), BF16, "vmem")], args, 1 << 18)
        source = exchange(parts, even_pairs)

    kernel = lambda *refs: last_sum_kernel(peers, *refs)
    outs = [((peers, 2 * share, D), BF16, "vmem"), ((share, LANES), F32, "any")]
    parts, gain_total = call(kernel, outs, (exchange_within(parts),), 1 << 18)
    outs = [((rows, D), BF16, "any")] * 2
    outputs, input_grad = call(finish_kernel, outs, (exchange_within(parts),), 1 << 18)
    totals = []
    for left, right in ((stored[0], stored[2]), (stored[1], stored[3])):
        shape = (left[0].shape[1], right[0].shape[1])
        scratch = [pltpu.VMEM((steps * rows, n), BF16) for n in shape]
        kernel = lambda *refs: update_kernel(steps, *refs)
        totals += call(kernel, [(shape, BF16, "any")], (*left, *right), steps * matmul, scratch=scratch)
    return (
        outputs[None],
        input_grad[None],
        totals[1][None],
        totals[0][None],
        gain_total.reshape(1, D),
    )


def solution(mesh):
    placed = (
        P("section", None, None),
        P("section", None, None),
        P(),
        P(),
        P("section", None, None, None),
        P("section", None),
        P("section", None, "mp"),
        P("section", "mp", None),
        P("section", None),
    )
    return jax.shard_map(
        local,
        mesh=mesh,
        in_specs=placed,
        out_specs=(
            P("section", None, None),
            P("section", None, None),
            P("section", None, "mp"),
            P("section", "mp", None),
            P("section", None),
        ),
        check_vma=False,
    )
```

```python
import jax
import jax.numpy as jnp
from jax import lax
from jax.experimental import pallas as pl
from jax.experimental.pallas import tpu as pltpu
from jax.sharding import PartitionSpec as P

D = 1024
EPSILON = 1e-06
BOTH = ("section", "mp")
BF16 = jnp.bfloat16
F32 = jnp.float32
LANES = 128
VMEM_LIMIT = 8 << 20
ROOT = 0.7978845608028654
CUBE = 0.044715


def pair_groups(sections, peers, first):
    groups = []
    for k in range(first, sections + first, 2):
        pair = (k % sections, (k + 1) % sections)
        groups.append([s * peers + m for s in pair for m in range(peers)])
    return groups


def times(left, right):
    return jnp.dot(left, right, preferred_element_type=F32)


def against_rows(left, right):
    return lax.dot_general(left, right, (((1,), (1,)), ((), ())), preferred_element_type=F32)


def across_rows(left, right):
    return lax.dot_general(left, right, (((0,), (0,)), ((), ())), preferred_element_type=F32)


def in_vmem(value):
    return pltpu.with_memory_space_constraint(value, pltpu.VMEM)


def call(kernel, outs, args, flops, smem=(), hbm=(), scratch=()):
    space = lambda k: pltpu.SMEM if k in smem else pltpu.HBM if k in hbm else pltpu.VMEM
    return pl.pallas_call(
        kernel,
        out_shape=[
            {"vmem": pltpu.VMEM, "hbm": pltpu.HBM, "any": jax.ShapeDtypeStruct}[place](shape, dtype)
            for shape, dtype, place in outs
        ],
        in_specs=[pl.BlockSpec(memory_space=space(k)) for k in range(len(args))],
        out_specs=[
            pl.BlockSpec(memory_space=pltpu.HBM if place == "hbm" else pltpu.VMEM) for _, _, place in outs
        ],
        scratch_shapes=list(scratch),
        compiler_params=pltpu.CompilerParams(vmem_limit_bytes=VMEM_LIMIT),
        cost_estimate=pl.CostEstimate(flops=flops, transcendentals=0, bytes_accessed=1 << 20),
    )(*args)


def normalize(rows, gain, weight_in):
    scaled = (rows * gain).astype(BF16)
    inverse = lax.rsqrt(jnp.sum(rows * rows, axis=1, keepdims=True) * (1.0 / D) + EPSILON)
    return scaled, inverse, times(scaled, weight_in)


def gelu_parts(preact):
    square = preact * preact
    tanh = jnp.tanh(ROOT * preact * (1.0 + CUBE * square))
    cdf = 0.5 + 0.5 * tanh
    return preact * cdf, cdf, tanh, square


def gelu_slope(preact, cdf, tanh, square):
    return cdf + (0.5 * ROOT) * preact * (1.0 - tanh * tanh) * (1.0 + (3.0 * CUBE) * square)


def flat(part):
    return part.astype(F32).reshape(part.shape[0] * part.shape[1], part.shape[2])


def first_kernel(peers, *refs):
    plan_hbm, stashed, rows_hbm, grads_hbm, gain_hbm, weight_in_hbm, weight_out_hbm, *feeds = refs[:9]
    parts_out, *kept = refs[9:15]
    feeds_out = refs[15:17]
    later = refs[17:-8]
    plan, rows_ref, grads_ref, gain_ref, weight_in, weight_out, slot_ref, sems = refs[-8:]
    count = iter(range(sems.shape[0]))

    def begin(source, target):
        copy = pltpu.make_async_copy(source, target, sems.at[next(count)])
        copy.start()
        return copy

    planned = begin(plan_hbm, plan)
    fetches = [
        begin(grads_hbm, grads_ref),
        begin(weight_out_hbm, weight_out),
        begin(gain_hbm, gain_ref),
        begin(rows_hbm, rows_ref),
        begin(weight_in_hbm, weight_in),
    ]
    share = feeds_out[0].shape[1]
    own = pl.multiple_of(lax.axis_index("mp") * share, share)
    others = [begin(feed.at[:, pl.ds(own, share), :], target) for feed, target in zip(feeds, feeds_out)]
    planned.wait()
    fetches.append(begin(stashed.at[plan[0, 0]], slot_ref))
    others += [begin(stashed.at[plan[0, 1 + k]], target) for k, target in enumerate(later)]

    def load_grads():
        for fetch in fetches[:2]:
            fetch.wait()
        return grads_ref[...].astype(F32)

    def load_inputs():
        for fetch in fetches[2:5]:
            fetch.wait()
        return rows_ref[...].astype(F32)

    def load_slot():
        fetches[5].wait()
        return slot_ref[...].astype(F32)

    results = both_ways(peers, load_grads, load_inputs, load_slot, gain_ref, weight_in, weight_out, kept)
    place(peers, parts_out, *results[:2])
    kept[4][...] = results[2]
    for other in others:
        other.wait()


def later_kernel(peers, last, *refs):
    received, slot_ref, gain_ref, weight_in, weight_out, *gains = refs[: -5 if last else -6]
    parts_out, *kept = refs[-5 if last else -6 :]
    forward, backward, gain_sum = both_ways(
        peers,
        lambda: flat(received[peers:]),
        lambda: flat(received[:peers]),
        lambda: slot_ref[...].astype(F32),
        gain_ref,
        weight_in,
        weight_out,
        kept,
    )
    if not last:
        place(peers, parts_out, forward, backward)
        kept[4][...] = gain_sum
        return
    share = forward.shape[1]
    parts_out[:, :share, :D] = forward
    parts_out[:, share:, :D] = backward
    for ref in gains:
        gain_sum = gain_sum + ref[...]
    stack = jnp.concatenate([gain_sum[:, k * LANES : (k + 1) * LANES] for k in range(D // LANES)], axis=0)
    high = stack.astype(BF16)
    low = (stack - high.astype(F32)).astype(BF16)
    for k in range(peers):
        parts_out[k, :share, D:] = high
        parts_out[k, share:, D:] = low


def place(peers, parts_out, forward, backward):
    parts_out[:peers] = backward
    parts_out[peers:] = forward


def both_ways(peers, load_grads, load_inputs, load_slot, gain_ref, weight_in, weight_out, kept):
    hidden_out, scaled_out, grads_out, update_out = kept[:4]
    grads = load_grads()
    grads_low = grads.astype(BF16)
    grads_out[...] = grads_low
    hidden_grad = against_rows(grads_low, weight_out[...])
    inputs = load_inputs()
    gain = gain_ref[...].astype(F32)
    portion = 1.0 / peers
    share = inputs.shape[0] // peers
    slot = load_slot()
    rows = inputs.shape[0]
    scaled, inverses, products = normalize(jnp.concatenate([inputs, slot], axis=0), gain, weight_in[...])
    inverse, projected = inverses[:rows], products[:rows]
    slot_scaled, slot_inverse, slot_projected = scaled[rows:], inverses[rows:], products[rows:]
    scaled_out[...] = slot_scaled

    slot_preact = slot_inverse * slot_projected
    slot_hidden, *about = gelu_parts(slot_preact)
    hidden_out[...] = slot_hidden.astype(BF16)
    pre_grad = hidden_grad * gelu_slope(slot_preact, *about)
    update = (slot_inverse * pre_grad).astype(BF16)
    update_out[...] = update
    input_part = against_rows(update, weight_in[...])
    inner = jnp.sum(pre_grad * slot_projected, axis=1, keepdims=True)
    factor = inner * slot_inverse * slot_inverse * slot_inverse * (-1.0 / D)
    gain_sum = jnp.sum(input_part * slot, axis=0, keepdims=True)
    backward = grads * portion + input_part * gain + factor * slot
    backward = backward.reshape(peers, share, D).astype(BF16)

    hidden = gelu_parts(inverse * projected)[0].astype(BF16)
    forward = times(hidden, weight_out[...]) + inputs * portion
    forward = forward.reshape(peers, share, D).astype(BF16)
    return forward, backward, gain_sum


def sum_kernel(peers, sections, step, received, feed_rows, feed_grads, spread_out):
    position = lax.axis_index("section")
    for start, edge, feed in ((0, 0, feed_rows), (peers, sections - 1, feed_grads)):
        total = received[start].astype(F32)
        for k in range(1, peers):
            total = total + received[start + k].astype(F32)
        total = jnp.where(position == edge, feed[step].astype(F32), total).astype(BF16)
        for k in range(peers):
            spread_out[start + k] = total


def last_sum_kernel(peers, received, spread_out, gain_out):
    total = received[0].astype(F32)
    for k in range(1, peers):
        total = total + received[k].astype(F32)
    piece = total[:, :D].astype(BF16)
    for k in range(peers):
        spread_out[k] = piece
    share = total.shape[0] // 2
    gain_out[...] = total[:share, D:] + total[share:, D:]


def update_kernel(steps, *refs):
    out, left, right = refs[-3:]
    rows = refs[0].shape[0]
    for step in range(steps):
        left[step * rows : (step + 1) * rows, :] = refs[step][...]
        right[step * rows : (step + 1) * rows, :] = refs[steps + step][...]
    out[...] = across_rows(left[...], right[...]).astype(BF16)


def finish_kernel(received, outputs, input_grad):
    share = received.shape[1] // 2
    outputs[...] = flat(received[:, :share]).astype(BF16)
    input_grad[...] = flat(received[:, share:]).astype(BF16)


def local(
    arrive_rows,
    arrive_grads,
    feed_rows,
    feed_grads,
    stashed_rows,
    slot_order,
    enter_weight,
    leave_weight,
    norm_gain,
):
    sections = lax.axis_size("section")
    peers = lax.axis_size("mp")
    even_pairs = pair_groups(sections, peers, 0)
    odd_pairs = pair_groups(sections, peers, 1)
    in_hbm = lambda value: pltpu.with_memory_space_constraint(value, pltpu.HBM)
    weights = (enter_weight[0], leave_weight[0])
    stashed = in_hbm(stashed_rows[0])
    steps, rows = stashed.shape[0], stashed.shape[1]
    width = enter_weight.shape[2]
    share = rows // peers
    matmul = 2 * rows * D * width

    def exchange(parts, groups):
        return in_vmem(lax.all_to_all(parts, BOTH, 0, 0, axis_index_groups=groups, tiled=True))

    def exchange_within(parts):
        return in_vmem(lax.all_to_all(parts, "mp", 0, 0, tiled=True))

    kept = [((rows, width), BF16), ((rows, D), BF16), ((rows, D), BF16), ((rows, width), BF16), ((1, D), F32)]
    stored = [[] for _ in kept]
    for step in range(steps):
        last = step + 1 == steps
        whole = (peers, 2 * share, D + LANES) if last else (2 * peers, share, D)
        outs = [(whole, BF16, "vmem")]
        outs += [(shape, dtype, "vmem") for shape, dtype in kept[: 4 if last else 5]]
        if step == 0:
            args = [slot_order, stashed, arrive_rows[0], arrive_grads[0], norm_gain, *weights, feed_rows, feed_grads]
            args = [in_hbm(arg) for arg in args]
            outs += [((steps - 1, share, D), BF16, "vmem")] * 2
            outs += [((rows, D), BF16, "vmem")] * (steps - 1)
            scratch = [pltpu.SMEM(slot_order.shape, jnp.int32)]
            scratch += [pltpu.VMEM(arg.shape, BF16) for arg in args[2:7]]
            scratch += [pltpu.VMEM((rows, D), BF16), pltpu.SemaphoreType.DMA((8 + steps,))]
            kernel = lambda *refs: first_kernel(peers, *refs)
            parts, *results = call(kernel, outs, args, 5 * matmul, hbm=range(len(args)), scratch=scratch)
            feeds, later = results[5:7], results[7:]
        else:
            args = [source, later[step - 1], in_vmem(norm_gain), *map(in_vmem, weights)]
            args += stored[4] if last else []
            kernel = lambda *refs: later_kernel(peers, last, *refs)
            parts, *results = call(kernel, outs, args, 5 * matmul)
        for past, result in zip(stored, results):
            past.append(result)
        if last:
            break
        kernel = lambda *refs: sum_kernel(peers, sections, step, *refs)
        args = (exchange(parts, odd_pairs), *feeds)
        (parts,) = call(kernel, [((2 * peers, share, D), BF16, "vmem")], args, 1 << 18)
        source = exchange(parts, even_pairs)

    kernel = lambda *refs: last_sum_kernel(peers, *refs)
    outs = [((peers, 2 * share, D), BF16, "vmem"), ((share, LANES), F32, "any")]
    parts, gain_total = call(kernel, outs, (exchange_within(parts),), 1 << 18)
    outs = [((rows, D), BF16, "any")] * 2
    outputs, input_grad = call(finish_kernel, outs, (exchange_within(parts),), 1 << 18)
    totals = []
    for left, right in ((stored[0], stored[2]), (stored[1], stored[3])):
        shape = (left[0].shape[1], right[0].shape[1])
        scratch = [pltpu.VMEM((steps * rows, n), BF16) for n in shape]
        kernel = lambda *refs: update_kernel(steps, *refs)
        totals += call(kernel, [(shape, BF16, "any")], (*left, *right), steps * matmul, scratch=scratch)
    return (
        outputs[None],
        input_grad[None],
        totals[1][None],
        totals[0][None],
        gain_total.reshape(1, D),
    )


def solution(mesh):
    placed = (
        P("section", None, None),
        P("section", None, None),
        P(),
        P(),
        P("section", None, None, None),
        P("section", None),
        P("section", None, "mp"),
        P("section", "mp", None),
        P("section", None),
    )
    return jax.shard_map(
        local,
        mesh=mesh,
        in_specs=placed,
        out_specs=(
            P("section", None, None),
            P("section", None, None),
            P("section", None, "mp"),
            P("section", "mp", None),
            P("section", None),
        ),
        check_vma=False,
    )
```
